32 devices in a mesh: gx: 4 (over x, core), gy: 2 (over y), gz: 4 (over z).
Axes of the slice: x: 2, y: 2, z: 4, core: 2. Of those that a mesh axis runs over, the one named last changes fastest.
Arguments:
- atom_embedding: bfloat16 [4, 2, 4, 64, 512], P('gx', 'gy', 'gz'), may hold values from -6 to 6
- output_adjoint: bfloat16 [4, 2, 4, 64, 512], P('gx', 'gy', 'gz'), may hold values from -6 to 6
- fractional_coords: float32 [4, 2, 4, 3, 512], P('gx', 'gy', 'gz'), may hold values from 0 to 1, as said below
- element_labels: int32 [4, 2, 4, 512], P('gx', 'gy', 'gz'), may hold values from 0 to 3
- adjacent_ghost_entries: int32 [4, 2, 4, 16, 512], P('gx', 'gy', 'gz'), may hold values from 0 to 13823, as said below
- miller_triples: int32 [3, 2048], replicated, may hold values from -8 to 8
- reciprocal_kernel: float32 [2048, 64], replicated, may hold values from 0.02 to 0.2
- channel_mixing_matrix: bfloat16 [64, 64], replicated, may hold values from -0.75 to 0.75
- element_channel_factor: float32 [4, 64], replicated, may hold values from 0.25 to 1.75
- distance_kernel: float32 [16, 64], replicated, may hold values from -1.5 to 1.5
Outputs:
- atom_grad: bfloat16 [4, 2, 4, 64, 512], P('gx', 'gy', 'gz')
- position_grad: float32 [4, 2, 4, 3, 512], P('gx', 'gy', 'gz')
- weight_grad: float32 [64, 64], replicated
- radial_grad: float32 [16, 64], replicated
- filter_grad: float32 [2048, 64], P(('gx', 'gy', 'gz'))
The draws below stay inside these ranges and needn't reach their ends.
Inputs may be any that keep to these rules, and one draw needn't show every extreme that they name: `adjacent_ghost_entries`: the atoms of a brick form 32 blocks of 16 in order; block q < 27 is the cell of offset (q // 9 - 1, (q // 3) % 3 - 1, q % 3 - 1) of the brick, blocks 27 to 31 lie in its central cell. A ghost entry e names atom e % 512 of slot e // 512; an entry in a slot of offset o names an atom of a block whose cell offset equals -o in every dimension where o is not zero, and o is zero in every dimension where the listing atom's cell offset is zero; every slot occurs. `fractional_coords`: an atom of a block whose cell offset is -1 or 1 in a dimension lies within a quarter of the brick length of that face in that dimension. `miller_triples`: integer components; any triple may occur, the zero triple too.
All inputs are finite; a program needn't handle non-finite values.
Results may differ from the reference program's by a relative error of at most 0.0053.
Values may be sent and summed in bfloat16 or wider, within the bound.
A program may use at most 128 MiB of HBM per device.

```python
import math
import jax
import jax.numpy as jnp
from jax import lax

ATOMS_DEV = 512
CH = 64
RECIP_POINTS = 2048
NBR = 16
NB = 16
KINDS = 4
MAX_RECIP_INDEX = 8
GX = 4
GY = 2
GZ = 4
N_GX = 4
N_GY = 2
N_GZ = 4


rim_width = 0.25


def block_cells():
    block_ids = jnp.arange(32, dtype=jnp.int32)
    first = jnp.where(block_ids < 27, block_ids // 9 - 1, 0)
    second = jnp.where(block_ids < 27, block_ids // 3 % 3 - 1, 0)
    third = jnp.where(block_ids < 27, block_ids % 3 - 1, 0)
    return jnp.stack([first, second, third], axis=1)


def atom_cells():
    atom_ids = jnp.arange(ATOMS_DEV, dtype=jnp.int32)
    return block_cells()[atom_ids // (ATOMS_DEV // 32)]


def draw_fractional_coords(key, part):
    cells = jnp.transpose(atom_cells(), (1, 0))
    uniform_part = jax.random.uniform(key, (GX, GY, GZ, 3, ATOMS_DEV), jnp.float32)
    low_side = rim_width * uniform_part
    high_side = 1.0 - rim_width + rim_width * uniform_part
    middle = rim_width + (1.0 - 2.0 * rim_width) * uniform_part
    return jnp.where(cells == -1, low_side, jnp.where(cells == 1, high_side, middle)).astype(jnp.float32)


def draw_adjacent_ghost_entries(key, part):
    key_cross = jax.random.fold_in(key, 11)
    key_centre = jax.random.fold_in(key, 12)
    key_atom = jax.random.fold_in(key, 13)
    array_dimensions = (GX, GY, GZ, NBR, ATOMS_DEV)
    cell_atoms = ATOMS_DEV // 32
    own_cell = jnp.transpose(atom_cells(), (1, 0))
    crossing = jax.random.randint(key_cross, (GX, GY, GZ, NBR, 3, ATOMS_DEV), 0, 2).astype(jnp.int32)
    offsets = own_cell * crossing
    target = jnp.where(offsets != 0, -own_cell, own_cell)
    slot_id = 9 * (offsets[:, :, :, :, 0] + 1) + 3 * (offsets[:, :, :, :, 1] + 1) + (offsets[:, :, :, :, 2] + 1)
    drawn_block = 9 * (target[:, :, :, :, 0] + 1) + 3 * (target[:, :, :, :, 1] + 1) + (target[:, :, :, :, 2] + 1)
    centre_pick = jax.random.randint(key_centre, array_dimensions, 0, 6).astype(jnp.int32)
    centre_block = jnp.where(centre_pick == 0, 13, 26 + centre_pick)
    target_block = jnp.where(drawn_block == 13, centre_block, drawn_block)
    atom_pick = jax.random.randint(key_atom, array_dimensions, 0, cell_atoms).astype(jnp.int32)
    return (slot_id * ATOMS_DEV + target_block * cell_atoms + atom_pick).astype(jnp.int32)


def touch_ends(drawn, rng, least, largest):
    index_at = [jax.random.randint(jax.random.fold_in(rng, axis), (), 0, length) for axis, length in enumerate(drawn.shape)]
    widest = drawn.shape.index(max(drawn.shape))
    neighbour = index_at[:widest] + [(index_at[widest] + 1) % drawn.shape[widest]] + index_at[widest + 1:]
    return drawn.at[tuple(index_at)].set(least).at[tuple(neighbour)].set(largest)


def level_of(own_key, shape, cuts, least, high):
    level = 1.0
    for axis_at, blocks in cuts:
        steps = jax.random.uniform(jax.random.fold_in(jax.random.fold_in(own_key, 6), axis_at), (blocks,), jnp.float32, least / len(cuts), high / len(cuts))
        level = level * jnp.repeat(jnp.exp(steps), shape[axis_at] // blocks).reshape((-1,) + (1,) * (len(shape) - 1 - axis_at))
    return level


def centred(key, shape, scale, bound, pieces=(), kind=jnp.bfloat16):
    result = jax.random.normal(key, shape, jnp.float32) * scale
    if len(pieces) > 0:
        result = level_of(key, shape, pieces, -0.22, 0.18) * result
    return jnp.clip(result, min=-bound, max=bound).astype(kind)


def setup_inputs(seed: int = 0) -> dict:
    arg_keys = jax.random.split(jax.random.key(seed), 11)
    return {
        "atom_embedding": centred(arg_keys[0], (GX, GY, GZ, CH, ATOMS_DEV), 1.0, 6.0, ((0, 4), (1, 2), (2, 4))),
        "output_adjoint": centred(arg_keys[1], (GX, GY, GZ, CH, ATOMS_DEV), 1.0, 6.0, ((0, 4), (1, 2), (2, 4))),
        "fractional_coords": draw_fractional_coords(jax.random.fold_in(arg_keys[10], 71), 0),
        "element_labels": touch_ends(jax.random.randint(arg_keys[3], (GX, GY, GZ, ATOMS_DEV), 0, KINDS), jax.random.fold_in(arg_keys[3], 1), 0, KINDS - 1).astype(jnp.int32),
        "adjacent_ghost_entries": draw_adjacent_ghost_entries(jax.random.fold_in(arg_keys[10], 71), 0),
        "miller_triples": touch_ends(jax.random.randint(arg_keys[5], (3, RECIP_POINTS), 0 - MAX_RECIP_INDEX, MAX_RECIP_INDEX + 1), jax.random.fold_in(arg_keys[5], 1), 0 - MAX_RECIP_INDEX, MAX_RECIP_INDEX).astype(jnp.int32),
        "reciprocal_kernel": jnp.clip(jnp.exp(jax.random.uniform(arg_keys[6], (RECIP_POINTS, CH), jnp.float32, math.log(0.02), math.log(0.2))), 0.02, 0.2),
        "channel_mixing_matrix": centred(arg_keys[7], (CH, CH), CH ** -0.5, 0.75),
        "element_channel_factor": jnp.clip(1.0 + 0.15 * jax.random.normal(arg_keys[8], (KINDS, CH), jnp.float32), 0.25, 1.75),
        "distance_kernel": centred(arg_keys[9], (NB, CH), NB ** -0.5, 1.5, (), jnp.float32),
    }


circle_angle = 2.0 * math.pi
reach_sq = 0.75

def phases(local_pos, anchor, reciprocal_points_rescaled):
    absolute = local_pos + anchor[:, None]
    angles = absolute[0][:, None] * reciprocal_points_rescaled[0][None, :]
    angles = angles + absolute[1][:, None] * reciprocal_points_rescaled[1][None, :]
    angles = angles + absolute[2][:, None] * reciprocal_points_rescaled[2][None, :]
    return (jnp.cos(angles).astype(jnp.bfloat16), jnp.sin(angles).astype(jnp.bfloat16))

def structure_terms(cos_part, sin_part, stacked):
    contract = (((0,), (1,)), ((), ()))
    with_cos = lax.dot_general(cos_part, stacked, contract, preferred_element_type=jnp.float32)
    with_sin = lax.dot_general(sin_part, stacked, contract, preferred_element_type=jnp.float32)
    return jnp.concatenate([with_cos, with_sin], axis=1)

def coefficients(totals, filt_rows, norm_atoms, norm_k):
    channels = filt_rows.shape[1]
    cos_struct = totals[:, 0:channels] * norm_atoms
    cos_back = totals[:, channels:2 * channels] * norm_k
    sin_struct = totals[:, 2 * channels:3 * channels] * norm_atoms
    sin_back = totals[:, 3 * channels:4 * channels] * norm_k
    coeffs = jnp.concatenate([norm_atoms * filt_rows * cos_back, norm_k * filt_rows * cos_struct, norm_atoms * filt_rows * sin_back, norm_k * filt_rows * sin_struct], axis=1)
    return (coeffs.astype(jnp.bfloat16), cos_struct * cos_back + sin_struct * sin_back)

def ewald_pieces(running, piece_rows, start_at, cos_all, sin_all, stacked, reciprocal_points_rescaled):
    count_rows = piece_rows.shape[0]
    channels = stacked.shape[0] // 2
    cos_part = lax.dynamic_slice_in_dim(cos_all, start_at, count_rows, 1)
    sin_part = lax.dynamic_slice_in_dim(sin_all, start_at, count_rows, 1)
    kv_part = lax.dynamic_slice_in_dim(reciprocal_points_rescaled, start_at, count_rows, 1)
    contract = (((0,), (1,)), ((), ()))
    atom_part = lax.dot_general(piece_rows[:, 0:channels], cos_part, contract, preferred_element_type=jnp.float32)
    atom_part = atom_part + lax.dot_general(piece_rows[:, 2 * channels:3 * channels], sin_part, contract, preferred_element_type=jnp.float32)
    along_u = lax.dot_general(stacked, piece_rows[:, 0:2 * channels], contract, preferred_element_type=jnp.float32)
    along_v = lax.dot_general(stacked, piece_rows[:, 2 * channels:4 * channels], contract, preferred_element_type=jnp.float32)
    angle_grad = along_v * cos_part.astype(jnp.float32) - along_u * sin_part.astype(jnp.float32)
    pos_part = lax.dot_general(kv_part, angle_grad, (((1,), (1,)), ((), ())), precision=lax.Precision.HIGHEST)
    return (running[0] + atom_part, running[1] + pos_part)

def species_gains(table, kinds):
    onehot = (kinds[None, :] == jnp.arange(table.shape[0], dtype=jnp.int32)[:, None]).astype(jnp.float32)
    return lax.dot_general(table, onehot, (((0,), (0,)), ((), ())), precision=lax.Precision.HIGHEST)

def offset_table():
    steps_one = jnp.arange(3, dtype=jnp.float32) - 1.0
    along_x = jnp.broadcast_to(steps_one[:, None, None], (3, 3, 3))
    along_y = jnp.broadcast_to(steps_one[None, :, None], (3, 3, 3))
    along_z = jnp.broadcast_to(steps_one[None, None, :], (3, 3, 3))
    return jnp.stack([along_x, along_y, along_z], axis=-1)

def short_range(ghost_values, ghost_places, neighbour_ids, radial_weights):
    channels = ghost_values.shape[1]
    flat_z = jnp.transpose(ghost_values, (1, 0, 2)).reshape(channels, -1)
    flat_pos = jnp.transpose(ghost_places, (1, 0, 2)).reshape(3, -1)
    near_z = flat_z[:, neighbour_ids]
    near_pos = flat_pos[:, neighbour_ids]
    relative = near_pos - ghost_places[13][:, None, :]
    dist_sq = lax.optimization_barrier(jnp.sum(relative * relative, axis=0))
    basis_count = radial_weights.shape[0]
    spacing = reach_sq / (basis_count - 1)
    centres = jnp.arange(basis_count, dtype=jnp.float32) * spacing
    radial_basis = jnp.exp(-jnp.square((dist_sq[None, :, :] - centres[:, None, None]) / (2.0 * spacing)))
    filters = jnp.einsum('bc,bja->cja', radial_weights, radial_basis, precision=lax.Precision.HIGHEST)
    agg = lax.optimization_barrier(jnp.sum(filters * near_z, axis=1)) * neighbour_ids.shape[0] ** (-0.5)
    return jax.nn.silu(agg)

def local_backward(ghost_z, ghost_pos, neighbour_ids, distance_kernel, upstream):

    def mapped(ghost_values, ghost_places, radial_weights):
        return short_range(ghost_values, ghost_places, neighbour_ids, radial_weights)
    _, pullback = jax.vjp(mapped, ghost_z.astype(jnp.float32), ghost_pos, distance_kernel)
    return pullback(upstream.astype(jnp.float32))

def fold_wrap(padded, along_axis):
    inner_size = padded.shape[along_axis] - 2
    interior = lax.slice_in_dim(padded, 1, inner_size + 1, axis=along_axis)
    low_plane = lax.slice_in_dim(padded, 0, 1, axis=along_axis)
    high_plane = lax.slice_in_dim(padded, inner_size + 1, inner_size + 2, axis=along_axis)
    middle_shape = list(low_plane.shape)
    middle_shape[along_axis] = inner_size - 2
    middle = jnp.zeros(middle_shape, padded.dtype)
    return interior + jnp.concatenate([high_plane, middle, low_plane], axis=along_axis)

def reference(atom_embedding, output_adjoint, fractional_coords, element_labels, adjacent_ghost_entries, miller_triples, reciprocal_kernel, channel_mixing_matrix, element_channel_factor, distance_kernel):
    brick_count = N_GX * N_GY * N_GZ
    atom_count = ATOMS_DEV
    norm_atoms = (atom_count * brick_count) ** (-0.5)
    norm_k = RECIP_POINTS ** (-0.5)
    accumulated_entries = jnp.array([N_GX, N_GY, N_GZ], jnp.float32)
    reciprocal_points_rescaled = miller_triples.astype(jnp.float32) * (circle_angle / accumulated_entries)[:, None]
    flat_h = atom_embedding.reshape(brick_count, CH, atom_count)
    flat_dy = output_adjoint.reshape(brick_count, CH, atom_count)
    flat_pos = fractional_coords.reshape(brick_count, 3, atom_count)
    flat_kind = element_labels.reshape(brick_count, atom_count)
    flat_nbr = adjacent_ghost_entries.reshape(brick_count, NBR, atom_count)
    indices = jnp.arange(brick_count, dtype=jnp.int32)

    def locate(brick_id):
        brick_id = brick_id.astype(jnp.int32)
        return ((brick_id // (N_GY * N_GZ)).astype(jnp.int32), (brick_id // N_GZ % N_GY).astype(jnp.int32), (brick_id % N_GZ).astype(jnp.int32))

    def anchor_of(brick_id):
        brick_x, brick_y, brick_z = locate(brick_id)
        return jnp.stack([brick_x, brick_y, brick_z]).astype(jnp.float32)

    def add_terms(totals, brick_id):
        cos_all, sin_all = phases(flat_pos[brick_id], anchor_of(brick_id), reciprocal_points_rescaled)
        stacked = jnp.concatenate([flat_h[brick_id], flat_dy[brick_id]], axis=0)
        return (totals + structure_terms(cos_all, sin_all, stacked), None)
    totals, _ = lax.scan(add_terms, jnp.zeros((RECIP_POINTS, 4 * CH), jnp.float32), indices)
    coeffs, filter_grad = coefficients(totals, reciprocal_kernel, norm_atoms, norm_k)

    def make_z(brick_id):
        gain_rows = species_gains(element_channel_factor, flat_kind[brick_id])
        projected = lax.dot_general(channel_mixing_matrix, flat_h[brick_id], (((0,), (0,)), ((), ())), preferred_element_type=jnp.float32)
        return ((projected * gain_rows).astype(jnp.bfloat16), gain_rows)
    zfeat, gains_all = lax.map(make_z, indices)
    pad_spec = ((1, 1), (1, 1), (1, 1), (0, 0), (0, 0))
    z_pad = jnp.pad(zfeat.reshape(N_GX, N_GY, N_GZ, CH, atom_count), pad_spec, mode='wrap')
    p_pad = jnp.pad(fractional_coords, pad_spec, mode='wrap')
    offsets = offset_table()[..., None]

    def brick_step(running, brick_id):
        grad_zpad, grad_ppad, grad_rad = running
        brick_x, brick_y, brick_z = locate(brick_id)
        zero_index = jnp.zeros((), jnp.int32)
        corner = (brick_x, brick_y, brick_z, zero_index, zero_index)
        ghost_z = lax.dynamic_slice(z_pad, corner, (3, 3, 3, CH, atom_count)).reshape(27, CH, atom_count)
        ghost_p = (lax.dynamic_slice(p_pad, corner, (3, 3, 3, 3, atom_count)) + offsets).reshape(27, 3, atom_count)
        grad_z, grad_p, grad_r = local_backward(ghost_z, ghost_p, flat_nbr[brick_id], distance_kernel, flat_dy[brick_id])
        region_z = lax.dynamic_slice(grad_zpad, corner, (3, 3, 3, CH, atom_count)) + grad_z.reshape(3, 3, 3, CH, atom_count)
        grad_zpad = lax.dynamic_update_slice(grad_zpad, region_z, corner)
        region_p = lax.dynamic_slice(grad_ppad, corner, (3, 3, 3, 3, atom_count)) + grad_p.reshape(3, 3, 3, 3, atom_count)
        grad_ppad = lax.dynamic_update_slice(grad_ppad, region_p, corner)
        cos_all, sin_all = phases(flat_pos[brick_id], anchor_of(brick_id), reciprocal_points_rescaled)
        stacked = jnp.concatenate([flat_h[brick_id], flat_dy[brick_id]], axis=0)
        zeros_pair = (jnp.zeros((CH, atom_count), jnp.float32), jnp.zeros((3, atom_count), jnp.float32))
        ewald_h, ewald_pos = ewald_pieces(zeros_pair, coeffs, zero_index, cos_all, sin_all, stacked, reciprocal_points_rescaled)
        return ((grad_zpad, grad_ppad, grad_rad + grad_r), (ewald_h, ewald_pos))
    start_state = (jnp.zeros((N_GX + 2, N_GY + 2, N_GZ + 2, CH, atom_count), jnp.float32), jnp.zeros((N_GX + 2, N_GY + 2, N_GZ + 2, 3, atom_count), jnp.float32), jnp.zeros((NB, CH), jnp.float32))
    (grad_zpad, grad_ppad, radial_grad), (ewald_h, ewald_pos) = lax.scan(brick_step, start_state, indices)
    zgrad = fold_wrap(fold_wrap(fold_wrap(grad_zpad, 0), 1), 2).reshape(brick_count, CH, atom_count)
    pos_short = fold_wrap(fold_wrap(fold_wrap(grad_ppad, 0), 1), 2).reshape(brick_count, 3, atom_count)
    zscaled = (zgrad * gains_all).astype(jnp.bfloat16)

    def finish(brick_id):
        atom_short = jnp.dot(channel_mixing_matrix, zscaled[brick_id], preferred_element_type=jnp.float32)
        atom_total = (flat_dy[brick_id].astype(jnp.float32) + ewald_h[brick_id] + atom_short).astype(jnp.bfloat16)
        weight_part = lax.dot_general(flat_h[brick_id], zscaled[brick_id], (((1,), (1,)), ((), ())), preferred_element_type=jnp.float32)
        return (atom_total, weight_part)
    atom_grad, weight_parts = lax.map(finish, indices)
    weight_grad = lax.optimization_barrier(jnp.sum(weight_parts, axis=0))
    position_grad = (ewald_pos + pos_short).reshape(fractional_coords.shape)
    return (atom_grad.reshape(atom_embedding.shape), position_grad, weight_grad, radial_grad, filter_grad)
```

```python
import functools
import itertools
import math

import jax
import jax.numpy as jnp
from jax import lax
from jax.experimental import pallas as pl
from jax.experimental.pallas import tpu as pltpu
from jax.sharding import PartitionSpec as P

AXES = ("gx", "gy", "gz")
reach_sq = 0.75
LANES = 128
VMEM_LIMIT = 60 * 1024 * 1024
f32 = jnp.float32
bf16 = jnp.bfloat16
NT = (((1,), (1,)), ((), ()))
OFFSETS = list(itertools.product((-1, 0, 1), repeat=3))
POS_HI, POS_MID, POS_LO, POS_OFF, LABEL = 64, 72, 80, 88, 96
GATHERED = 96


def dot(a, b):
    return jnp.dot(a, b, preferred_element_type=f32)


def dot_nt(a, b):
    return lax.dot_general(a, b, NT, preferred_element_type=f32)


def split2(x):
    hi = x.astype(bf16)
    return hi, (x - hi.astype(f32)).astype(bf16)


def sincos_turns(u):
    q = jnp.round(u * 2.0)
    x = (u - 0.5 * q) * (2.0 * math.pi)
    odd = q - 2.0 * jnp.floor(q * 0.5)
    sign = 1.0 - 2.0 * odd
    y = x * x
    s = -1.0 / 39916800.0
    for c in (1.0 / 362880.0, -1.0 / 5040.0, 1.0 / 120.0, -1.0 / 6.0, 1.0):
        s = s * y + c
    c_ = 1.0 / 479001600.0
    for c in (-1.0 / 3628800.0, 1.0 / 40320.0, -1.0 / 720.0, 1.0 / 24.0, -0.5, 1.0):
        c_ = c_ * y + c
    return c_ * sign, s * x * sign


def phase_kernel(h_ref, dy_ref, pos_ref, turns_ref, label_ref, mil_ref,
                 cos_ref, sin_ref, part_ref, table_ref):
    channels, atoms = h_ref.shape
    rows = mil_ref.shape[0]
    step = 128
    h = h_ref[...]
    stacked = jnp.concatenate([h, dy_ref[...]], axis=0)
    pos = pos_ref[...]
    hi = pos.astype(bf16).astype(f32)
    mid = (pos - hi).astype(bf16).astype(f32)
    lo = pos - hi - mid
    blank = jnp.zeros((LANES - LABEL - 8, atoms), f32)
    feats = jnp.concatenate(
        [h.astype(f32), hi, mid, lo, jnp.zeros((8, atoms), f32), label_ref[...], blank], axis=0)
    table_ref[...] = jnp.transpose(feats).astype(bf16).reshape(table_ref.shape)
    w0, w1, w2 = turns_ref[0:1, :], turns_ref[1:2, :], turns_ref[2:3, :]

    def body(i, _):
        at = pl.ds(pl.multiple_of(i * step, step), step)
        m = mil_ref[at, :]
        u = m[:, 0:1] * w0 + m[:, 1:2] * w1 + m[:, 2:3] * w2
        c, s = sincos_turns(u)
        c = c.astype(bf16)
        s = s.astype(bf16)
        cos_ref[at, :] = c
        sin_ref[at, :] = s
        part_ref[at, 0:2 * channels] = dot_nt(c, stacked).astype(bf16)
        part_ref[at, 2 * channels:4 * channels] = dot_nt(s, stacked).astype(bf16)
        return 0

    lax.fori_loop(0, rows // step, body, 0)


def coords(linear, sizes):
    nx, ny, nz = sizes
    return (linear // (ny * nz), (linear // nz) % ny, linear % nz)


def my_linear(sizes):
    nx, ny, nz = sizes
    return (lax.axis_index("gx") * ny + lax.axis_index("gy")) * nz + lax.axis_index("gz")


def neighbour(offset, sizes, flip):
    return tuple(
        lax.rem(lax.axis_index(a) + (n - flip * o), n) if flip > 0
        else lax.rem(lax.axis_index(a) + (n + o), n)
        for a, o, n in zip(AXES, offset, sizes))


def enter(n, sizes):
    me = my_linear(sizes)
    barrier = pltpu.get_barrier_semaphore()

    def signal(i, _):
        pl.semaphore_signal(barrier, inc=1, device_id=coords(lax.rem(me + i, n), sizes),
                            device_id_type=pl.DeviceIdType.MESH)
        return 0

    lax.fori_loop(1, n, signal, 0)
    pl.semaphore_wait(barrier, n - 1)
    return me


def span(o, low, high):
    return pl.ds(1, 3) if o == 0 else pl.ds(high if o > 0 else low, 1)


def own_span(o):
    return pl.ds(0, 3) if o == 0 else pl.ds(0 if o > 0 else 2, 1)


def local_span(o):
    return pl.ds(0, 3 if o == 0 else 1)


def all_bytes(ref, n, sem):
    part = ref.at[pl.ds(0, n - 1)]
    return pltpu.make_async_copy(part, part, sem)


def gather_kernel(sizes, norm_atoms, norm_k, table_ref, part_ref, kf_ref,
                  ext_ref, coef_ref, fg_ref, halo, recv, hs, hr, ss, rs):
    n = sizes[0] * sizes[1] * sizes[2]
    me = enter(n, sizes)
    copies = []
    for o in OFFSETS:
        if o == (0, 0, 0):
            continue
        src = table_ref.at[tuple(own_span(d) for d in o)]
        dst = halo.at[tuple(span(d, 0, 4) for d in o)]
        slot = 9 * (o[0] + 1) + 3 * (o[1] + 1) + o[2] + 1
        copy = pltpu.make_async_remote_copy(
            src_ref=src, dst_ref=dst, send_sem=hs.at[slot], recv_sem=hr.at[slot],
            device_id=neighbour(o, sizes, 1), device_id_type=pl.DeviceIdType.MESH)
        copy.start()
        copies.append(copy)

    def send(i, _):
        to = lax.rem(me + i, n)
        pltpu.make_async_remote_copy(
            src_ref=part_ref.at[to], dst_ref=recv.at[i - 1], send_sem=ss, recv_sem=rs,
            device_id=coords(to, sizes), device_id_type=pl.DeviceIdType.MESH).start()
        return 0

    lax.fori_loop(1, n, send, 0)
    for copy in copies:
        copy.wait()
    ext_ref[...] = halo[...]
    ext_ref[1:4, 1:4, 1:4] = table_ref[...]
    all_bytes(part_ref, n, ss).wait()
    all_bytes(recv, n, rs).wait()

    def add(i, total):
        return total + recv[i].astype(f32)

    total = lax.fori_loop(0, n - 1, add, part_ref[me].astype(f32))
    ch = kf_ref.shape[1]
    kf = kf_ref[...]
    cs = total[:, 0:ch] * norm_atoms
    cb = total[:, ch:2 * ch] * norm_k
    sst = total[:, 2 * ch:3 * ch] * norm_atoms
    sb = total[:, 3 * ch:4 * ch] * norm_k
    coef_ref[...] = jnp.concatenate(
        [norm_atoms * kf * cb, norm_k * kf * cs, norm_atoms * kf * sb, norm_k * kf * sst],
        axis=1).astype(bf16)
    fg_ref[...] = cs * cb + sst * sb


def short_kernel(basis_count, ext_ref, extra_ref, cid_ref, pos_ref, dy_ref, mix_ref, gain_ref,
                 shift_ref, dk_ref, dkt_ref, grad_ref, own_ref, wr_ref,
                 oh, near, filt, vals, ht, zg, acc, agg, gout, psum, rad):
    ep = oh.shape[1]
    nbr, atoms = cid_ref.shape
    channels = dy_ref.shape[0]
    cells = 125 * 16
    extras = extra_ref.shape[0] * 16
    pad = ep - cells - extras
    table = jnp.concatenate(
        [ext_ref[...].reshape(cells, LANES), extra_ref[...].reshape(extras, LANES),
         jnp.zeros((pad, LANES), bf16)], axis=0)
    tf = table.astype(f32)
    label = tf[:, LABEL:LABEL + 1]
    gains = jnp.zeros((ep, LANES), f32)
    for s in range(gain_ref.shape[0]):
        gains = jnp.where(label == float(s), gain_ref[s:s + 1, :], gains)
    zg[...] = gains
    z = dot(table, mix_ref[...]) * gains
    lane = lax.broadcasted_iota(jnp.int32, (ep, LANES), 1)
    full = jnp.where(lane < channels, z, tf) + shift_ref[...]
    vals[...] = jnp.transpose(full).astype(bf16)
    ht[...] = jnp.transpose(tf).astype(bf16)
    spacing = reach_sq / (basis_count - 1)
    centre = lax.broadcasted_iota(jnp.int32, (basis_count, 1), 0).astype(f32) * spacing
    inv = 1.0 / (2.0 * spacing)
    own = pos_ref[...]
    agg[...] = jnp.zeros_like(agg)
    psum[...] = jnp.zeros_like(psum)
    acc[...] = jnp.zeros_like(acc)
    rad[...] = jnp.zeros_like(rad)
    one, nil = jnp.ones((), bf16), jnp.zeros((), bf16)
    dkt_hi, dkt_lo = split2(dkt_ref[...])
    dkt3 = jnp.concatenate([dkt_hi, dkt_lo, dkt_hi], axis=1)
    dk_hi, dk_lo = split2(dk_ref[...])
    dk3 = jnp.concatenate([dk_hi, dk_lo, dk_hi], axis=1)
    tile = 256

    def geometry(j):
        at = near[j]
        place = at[POS_HI:POS_HI + 8] + at[POS_MID:POS_MID + 8] + at[POS_LO:POS_LO + 8]
        rel = (place + at[POS_OFF:POS_OFF + 8]) - own
        d2 = jnp.sum(rel * rel, axis=0, keepdims=True)
        arg = (d2 - centre) * inv
        return at, rel, arg, jnp.exp(-(arg * arg))

    def forward(j, _):
        cid = cid_ref[pl.ds(j, 1), :]
        high = cid // tile
        low = cid - high * tile
        for start in range(0, ep, tile):
            size = min(tile, ep - start)
            want = jnp.where(high == start // tile, low, -1).astype(f32).astype(bf16)
            rows = lax.broadcasted_iota(jnp.int32, (size, atoms), 0).astype(f32).astype(bf16)
            oh[j, start:start + size, :] = jnp.where(rows == want, one, nil)
        near[j] = dot(vals[0:GATHERED, :], oh[j])
        at, rel, arg, basis = geometry(j)
        b_hi, b_lo = split2(basis)
        f = dot(dkt3, jnp.concatenate([b_hi, b_hi, b_lo], axis=0))
        filt[j] = f
        agg[...] += f * at[0:channels]
        return 0

    lax.fori_loop(0, nbr, forward, 0)
    scale = nbr ** (-0.5)
    v = agg[...] * scale
    sg = 1.0 / (1.0 + jnp.exp(-v))
    gout[...] = dy_ref[...].astype(f32) * (sg * (1.0 + v * (1.0 - sg))) * scale

    def backward(j, _):
        g = gout[...]
        at, rel, arg, basis = geometry(j)
        dz = (filt[j] * g).astype(bf16)
        df_hi, df_lo = split2(at[0:channels] * g)
        db = dot(dk3, jnp.concatenate([df_hi, df_hi, df_lo], axis=0))
        dd2 = jnp.sum(db * basis * arg, axis=0, keepdims=True) * (-2.0 * inv)
        drel = 2.0 * rel * dd2
        psum[...] += drel
        d_hi = drel.astype(bf16).astype(f32)
        dvals = jnp.concatenate(
            [dz, jnp.concatenate([d_hi, drel - d_hi], axis=0).astype(bf16)], axis=0)
        acc[...] += dot_nt(oh[j], dvals)
        b_hi, b_lo = split2(basis)
        rad[...] += dot_nt(jnp.concatenate([b_hi, b_lo, b_hi], axis=1),
                           jnp.concatenate([df_hi, df_hi, df_lo], axis=1))
        return 0

    lax.fori_loop(0, nbr, backward, 0)
    g = acc[...]
    zgrad = g[:, 0:channels]
    pg = g[:, channels:channels + 8] + g[:, channels + 8:channels + 16]
    p_hi = pg.astype(bf16).astype(f32)
    grad_ref[...] = jnp.concatenate(
        [zgrad, p_hi, pg - p_hi, jnp.zeros((ep, LANES - channels - 16), f32)],
        axis=1).astype(bf16).reshape(grad_ref.shape)
    own_ref[...] = psum[...]
    scaled = (zgrad * zg[:, 0:channels]).astype(bf16)
    w = dot(ht[0:channels, :], scaled)
    half = channels // 2
    r = rad[...]
    hb = basis_count // 2
    wr_ref[...] = jnp.concatenate(
        [jnp.concatenate([w[:half], w[half:]], axis=1),
         jnp.concatenate([r[:hb], r[hb:]], axis=1),
         jnp.zeros((wr_ref.shape[0] - half - hb, LANES), f32)], axis=0).astype(bf16)


def return_kernel(sizes, channels, basis_count, grad_ref, coef_ref, wr_ref,
                  home_ref, extra_ref, coefs_ref, weight_ref, radial_ref,
                  back, crecv, wrecv, hs, hr, cs, cr, ws, wrs):
    n = sizes[0] * sizes[1] * sizes[2]
    me = enter(n, sizes)
    copies = []
    for o in OFFSETS:
        if o == (0, 0, 0):
            continue
        slot = 9 * (o[0] + 1) + 3 * (o[1] + 1) + o[2] + 1
        copy = pltpu.make_async_remote_copy(
            src_ref=grad_ref.at[tuple(span(d, 0, 4) for d in o)],
            dst_ref=back.at[(slot,) + tuple(local_span(d) for d in o)],
            send_sem=hs.at[slot], recv_sem=hr.at[slot],
            device_id=neighbour(o, sizes, -1), device_id_type=pl.DeviceIdType.MESH)
        copy.start()
        copies.append((o, slot, copy))

    def send(i, _):
        to = coords(lax.rem(me + i, n), sizes)
        pltpu.make_async_remote_copy(
            src_ref=coef_ref.at[0], dst_ref=crecv.at[i - 1], send_sem=cs, recv_sem=cr,
            device_id=to, device_id_type=pl.DeviceIdType.MESH).start()
        pltpu.make_async_remote_copy(
            src_ref=wr_ref.at[0], dst_ref=wrecv.at[i - 1], send_sem=ws, recv_sem=wrs,
            device_id=to, device_id_type=pl.DeviceIdType.MESH).start()
        return 0

    lax.fori_loop(1, n, send, 0)
    home_ref[...] = grad_ref[1:4, 1:4, 1:4].astype(f32)
    for o, slot, copy in copies:
        copy.wait()
        at = tuple(slice(0, 3) if d == 0 else (slice(0, 1) if d > 0 else slice(2, 3)) for d in o)
        loc = (slot,) + tuple(slice(0, 3 if d == 0 else 1) for d in o)
        home_ref[at] += back[loc].astype(f32)
    all_bytes(wrecv, n, ws).wait()
    all_bytes(wrecv, n, wrs).wait()
    all_bytes(crecv, n, cs).wait()
    all_bytes(crecv, n, cr).wait()
    wrecv[n - 1] = wr_ref[0]

    def add(i, total):
        return total + wrecv[lax.rem(me - i + n + n - 1, n)].astype(f32)

    total = lax.fori_loop(0, n, add, jnp.zeros(wr_ref.shape[1:], f32))
    half, hb = channels // 2, basis_count // 2
    weight_ref[0:half] = total[0:half, 0:channels]
    weight_ref[half:channels] = total[0:half, channels:2 * channels]
    radial_ref[0:hb] = total[half:half + hb, 0:channels]
    radial_ref[hb:basis_count] = total[half:half + hb, channels:2 * channels]
    coefs_ref[me] = coef_ref[0]

    def place(i, _):
        coefs_ref[lax.rem(me - i + n, n)] = crecv[i - 1]
        return 0

    lax.fori_loop(1, n, place, 0)


def final_kernel(coef_ref, cos_ref, sin_ref, h_ref, dy_ref, milt_ref, turn_ref, home_ref,
                 extra_ref, own_ref, gain_ref, mix_ref, atom_ref, pos_ref, eh, ep_):
    rows = coef_ref.shape[0]
    channels, atoms = h_ref.shape
    step = 256
    stacked = jnp.concatenate([h_ref[...], dy_ref[...]], axis=0)
    eh[...] = jnp.zeros_like(eh)
    ep_[...] = jnp.zeros_like(ep_)

    def body(i, _):
        at = pl.ds(pl.multiple_of(i * step, step), step)
        piece = coef_ref[at, :]
        c, s = cos_ref[at, :], sin_ref[at, :]
        turned = jnp.transpose(piece.astype(f32)).astype(bf16)
        eh[...] += dot(turned[0:channels], c) + dot(turned[2 * channels:3 * channels], s)
        u = dot(piece[:, 0:2 * channels], stacked)
        v = dot(piece[:, 2 * channels:4 * channels], stacked)
        hi, lo = split2(v * c.astype(f32) - u * s.astype(f32))
        m = milt_ref[i]
        ep_[...] += dot(m, hi) + dot(m, lo)
        return 0

    lax.fori_loop(0, rows // step, body, 0)
    blocks = 27 * 16
    home = jnp.concatenate(
        [home_ref[...].reshape(blocks, LANES),
         extra_ref[...].astype(f32).reshape(atoms - blocks, LANES)], axis=0)
    g = jnp.transpose(home)
    zscaled = (g[0:channels] * gain_ref[...]).astype(bf16)
    short = dot(mix_ref[...], zscaled)
    atom_ref[...] = (dy_ref[...].astype(f32) + eh[...] + short).astype(bf16)
    pos_short = g[channels:channels + 8] + g[channels + 8:channels + 16] - own_ref[...]
    pos_ref[...] = ep_[0:8] * turn_ref[...] + pos_short


def vmem(count):
    return [pl.BlockSpec(memory_space=pltpu.VMEM)] * count


def params(**more):
    return pltpu.CompilerParams(vmem_limit_bytes=VMEM_LIMIT, **more)


def shards(sizes, atom_embedding, output_adjoint, fractional_coords, element_labels,
           adjacent_ghost_entries, miller_triples, reciprocal_kernel, channel_mixing_matrix,
           element_channel_factor, distance_kernel):
    n = sizes[0] * sizes[1] * sizes[2]
    shape = jax.ShapeDtypeStruct
    h = atom_embedding[0, 0, 0]
    dy = output_adjoint[0, 0, 0]
    pos = fractional_coords[0, 0, 0]
    channels, atoms = h.shape
    rows = miller_triples.shape[1]
    share = rows // n
    basis_count = distance_kernel.shape[0]
    norm_atoms = (atoms * n) ** (-0.5)
    norm_k = rows ** (-0.5)
    counts = jnp.array(sizes, f32)
    anchor = jnp.stack([lax.axis_index(a) for a in AXES]).astype(f32)
    pos8 = jnp.pad(pos, ((0, 5), (0, 0)))
    turns8 = jnp.pad((pos + anchor[:, None]) / counts[:, None], ((0, 5), (0, 0)))
    labels = element_labels[0, 0, 0]
    label8 = jnp.pad(labels.astype(f32)[None, :], ((0, 7), (0, 0)))
    miller = miller_triples.astype(f32)
    mil8 = jnp.pad(miller.T, ((0, 0), (0, 5)))
    cos_all, sin_all, part, table = pl.pallas_call(
        phase_kernel,
        out_shape=(shape((rows, atoms), bf16), shape((rows, atoms), bf16),
                   shape((rows, 4 * channels), bf16), shape((atoms // 16, 16, LANES), bf16)),
        in_specs=vmem(6), out_specs=tuple(vmem(4)), compiler_params=params(), name="phases",
    )(h, dy, pos8, turns8, label8, mil8)

    me = lax.axis_index(AXES)
    kf = lax.dynamic_slice_in_dim(reciprocal_kernel, me * share, share, 0)
    dma = pltpu.SemaphoreType.DMA
    ext, coef, filter_share = pl.pallas_call(
        functools.partial(gather_kernel, sizes, norm_atoms, norm_k),
        out_shape=(shape((5, 5, 5, 16, LANES), bf16), shape((share, 4 * channels), bf16),
                   shape((share, channels), f32)),
        in_specs=vmem(3), out_specs=tuple(vmem(3)),
        scratch_shapes=[pltpu.VMEM((5, 5, 5, 16, LANES), bf16),
                        pltpu.VMEM((n, share, 4 * channels), bf16),
                        dma((27,)), dma((27,)), dma, dma],
        compiler_params=params(collective_id=0, has_side_effects=True), name="halo",
    )(table[:27].reshape(3, 3, 3, 16, LANES), part.reshape(n, share, 4 * channels), kf)

    e = adjacent_ghost_entries[0, 0, 0]
    slot, atom = e // atoms, e % atoms
    block = atom // 16
    cell = [slot // 9 - 1, (slot // 3) % 3 - 1, slot % 3 - 1]
    sub = [block // 9 - 1, (block // 3) % 3 - 1, block % 3 - 1]
    x, y, z = [t + 3 * o + 2 for t, o in zip(sub, cell)]
    place = jnp.where(block < 27, 25 * x + 5 * y + z, 125 + block - 27)
    cid = place * 16 + atom % 16
    nbr = e.shape[0]
    total = (125 + atoms // 16 - 27) * 16
    ep = -(-total // LANES) * LANES
    import numpy as np
    shift = np.zeros((ep, LANES), np.float32)
    for i, (cx, cy, cz) in enumerate(itertools.product(range(5), repeat=3)):
        for d, q in enumerate((cx, cy, cz)):
            shift[16 * i:16 * i + 16, POS_OFF + d] = -1.0 if q == 0 else (1.0 if q == 4 else 0.0)
    mixp = jnp.pad(channel_mixing_matrix, ((0, LANES - channels), (0, LANES - channels)))
    gainp = jnp.pad(element_channel_factor, ((0, 0), (0, LANES - channels)))
    wr_rows = -(-(channels // 2 + basis_count // 2) // 16) * 16
    grad, own, wr = pl.pallas_call(
        functools.partial(short_kernel, basis_count),
        out_shape=(shape((ep // 16, 16, LANES), bf16), shape((8, atoms), f32),
                   shape((wr_rows, LANES), bf16)),
        in_specs=vmem(10), out_specs=tuple(vmem(3)),
        scratch_shapes=[pltpu.VMEM((nbr, ep, atoms), bf16),
                        pltpu.VMEM((nbr, GATHERED, atoms), f32),
                        pltpu.VMEM((nbr, channels, atoms), f32),
                        pltpu.VMEM((LANES, ep), bf16), pltpu.VMEM((LANES, ep), bf16),
                        pltpu.VMEM((ep, LANES), f32),
                        pltpu.VMEM((ep, channels + 16), f32),
                        pltpu.VMEM((channels, atoms), f32), pltpu.VMEM((channels, atoms), f32),
                        pltpu.VMEM((8, atoms), f32), pltpu.VMEM((basis_count, channels), f32)],
        compiler_params=params(), name="short",
    )(ext, table[27:], cid, pos8, dy, mixp, gainp, jnp.asarray(shift), distance_kernel,
      distance_kernel.T)

    extras = atoms // 16 - 27
    home, coefs, weight_grad, radial_grad = pl.pallas_call(
        lambda g, c, w, a, b, r, s, *rest: return_kernel(
            sizes, channels, basis_count, g, c, w, a, None, b, r, s, *rest),
        out_shape=(shape((3, 3, 3, 16, LANES), f32), shape((n, share, 4 * channels), bf16),
                   shape((channels, channels), f32), shape((basis_count, channels), f32)),
        in_specs=vmem(3), out_specs=tuple(vmem(4)),
        scratch_shapes=[pltpu.VMEM((27, 3, 3, 3, 16, LANES), bf16),
                        pltpu.VMEM((n - 1, share, 4 * channels), bf16),
                        pltpu.VMEM((n, wr_rows, LANES), bf16),
                        dma((27,)), dma((27,)), dma, dma, dma, dma],
        compiler_params=params(collective_id=1, has_side_effects=True), name="home",
    )(grad[:125].reshape(5, 5, 5, 16, LANES), coef[None], wr[None])

    onehot = (labels[None, :] == jnp.arange(element_channel_factor.shape[0])[:, None])
    gains = lax.dot_general(element_channel_factor, onehot.astype(f32), (((0,), (0,)), ((), ())),
                            precision=lax.Precision.HIGHEST)
    milt = jnp.pad(miller.astype(bf16), ((0, 13), (0, 0)))
    milt = jnp.transpose(milt.reshape(16, rows // 256, 256), (1, 0, 2))
    turn = jnp.pad((2.0 * math.pi) / counts, (0, 5))[:, None] * jnp.ones((1, atoms), f32)
    atom_grad, pos_grad = pl.pallas_call(
        final_kernel,
        out_shape=(shape((channels, atoms), bf16), shape((8, atoms), f32)),
        in_specs=vmem(12), out_specs=tuple(vmem(2)),
        scratch_shapes=[pltpu.VMEM((channels, atoms), f32), pltpu.VMEM((16, atoms), f32)],
        compiler_params=params(), name="final",
    )(coefs.reshape(rows, 4 * channels), cos_all, sin_all, h, dy, milt, turn, home,
      grad[125:125 + extras], own, gains, channel_mixing_matrix)
    return (atom_grad[None, None, None], pos_grad[None, None, None, 0:3], weight_grad,
            radial_grad, filter_share)


def solution(mesh):
    sizes = tuple(mesh.shape[a] for a in AXES)
    brick = P("gx", "gy", "gz", None, None)
    return jax.shard_map(
        functools.partial(shards, sizes),
        mesh=mesh,
        in_specs=(brick, brick, brick, P("gx", "gy", "gz", None), brick,
                  P(), P(), P(), P(), P()),
        out_specs=(brick, brick, P(), P(), P(("gx", "gy", "gz"), None)),
        check_vma=False,
    )
```

```python
import functools
import itertools
import math

import jax
import jax.numpy as jnp
import numpy as np
from jax import lax
from jax.experimental import pallas as pl
from jax.experimental.pallas import tpu as pltpu
from jax.sharding import PartitionSpec as P

AXES = ("gx", "gy", "gz")
reach_sq = 0.75
LANES = 128
VMEM_LIMIT = 60 * 1024 * 1024
f32 = jnp.float32
bf16 = jnp.bfloat16
NT = (((1,), (1,)), ((), ()))
OFFSETS = list(itertools.product((-1, 0, 1), repeat=3))
POS_HI, POS_MID, POS_LO, POS_OFF, LABEL = 64, 72, 80, 88, 96
GATHERED = 96


def dot(a, b):
    return jnp.dot(a, b, preferred_element_type=f32)


def dot_nt(a, b):
    return lax.dot_general(a, b, NT, preferred_element_type=f32)


def split2(x):
    hi = x.astype(bf16)
    return hi, (x - hi.astype(f32)).astype(bf16)


def sincos_turns(u):
    q = jnp.round(u * 2.0)
    x = (u - 0.5 * q) * (2.0 * math.pi)
    odd = q - 2.0 * jnp.floor(q * 0.5)
    sign = 1.0 - 2.0 * odd
    y = x * x
    s = -1.0 / 39916800.0
    for c in (1.0 / 362880.0, -1.0 / 5040.0, 1.0 / 120.0, -1.0 / 6.0, 1.0):
        s = s * y + c
    c_ = 1.0 / 479001600.0
    for c in (-1.0 / 3628800.0, 1.0 / 40320.0, -1.0 / 720.0, 1.0 / 24.0, -0.5, 1.0):
        c_ = c_ * y + c
    return c_ * sign, s * x * sign


def phase_kernel(h_ref, dy_ref, geo_ref, mil_ref,
                 cos_ref, sin_ref, part_ref, table_ref, extra_ref):
    channels, atoms = h_ref.shape
    rows = mil_ref.shape[0]
    step = 128
    h = h_ref[...]
    stacked = jnp.concatenate([h, dy_ref[...]], axis=0)
    pos = geo_ref[0:8, :]
    hi = pos.astype(bf16).astype(f32)
    mid = (pos - hi).astype(bf16).astype(f32)
    lo = pos - hi - mid
    blank = jnp.zeros((LANES - LABEL - 8, atoms), f32)
    feats = jnp.concatenate(
        [h.astype(f32), hi, mid, lo, jnp.zeros((8, atoms), f32), geo_ref[16:24, :], blank], axis=0)
    table = jnp.transpose(feats).astype(bf16)
    inner = 27 * 16
    table_ref[...] = table[:inner].reshape(table_ref.shape)
    extra_ref[...] = table[inner:].reshape(extra_ref.shape)
    w0, w1, w2 = geo_ref[8:9, :], geo_ref[9:10, :], geo_ref[10:11, :]

    def body(i, _):
        at = pl.ds(pl.multiple_of(i * step, step), step)
        m = mil_ref[at, :]
        u = m[:, 0:1] * w0 + m[:, 1:2] * w1 + m[:, 2:3] * w2
        c, s = sincos_turns(u)
        c = c.astype(bf16)
        s = s.astype(bf16)
        cos_ref[at, :] = c
        sin_ref[at, :] = s
        part_ref[at, 0:2 * channels] = dot_nt(c, stacked).astype(bf16)
        part_ref[at, 2 * channels:4 * channels] = dot_nt(s, stacked).astype(bf16)
        return 0

    lax.fori_loop(0, rows // step, body, 0)


def coords(linear, sizes):
    nx, ny, nz = sizes
    return (linear // (ny * nz), (linear // nz) % ny, linear % nz)


def my_linear(sizes):
    nx, ny, nz = sizes
    return (lax.axis_index("gx") * ny + lax.axis_index("gy")) * nz + lax.axis_index("gz")


def neighbour(offset, sizes, sign):
    return tuple(lax.rem(lax.axis_index(a) + (n + sign * o), n)
                 for a, o, n in zip(AXES, offset, sizes))


def enter(n, sizes):
    me = my_linear(sizes)
    barrier = pltpu.get_barrier_semaphore()

    def signal(i, _):
        pl.semaphore_signal(barrier, inc=1, device_id=coords(lax.rem(me + i, n), sizes),
                            device_id_type=pl.DeviceIdType.MESH)
        return 0

    lax.fori_loop(1, n, signal, 0)
    pl.semaphore_wait(barrier, n - 1)
    return me


def span(o):
    return pl.ds(1, 3) if o == 0 else pl.ds(4 if o > 0 else 0, 1)


def own_span(o):
    return pl.ds(0, 3) if o == 0 else pl.ds(0 if o > 0 else 2, 1)


def remote(src, dst, send, recv, to):
    return pltpu.make_async_remote_copy(
        src_ref=src, dst_ref=dst, send_sem=send, recv_sem=recv, device_id=to,
        device_id_type=pl.DeviceIdType.MESH)


def all_bytes(ref, count, sem):
    part = ref.at[pl.ds(0, count)]
    return pltpu.make_async_copy(part, part, sem)


def stage_orders(sizes):
    bits = [[(i, k) for k in range(n.bit_length() - 1)] for i, n in enumerate(sizes)]
    first = bits[0] + bits[1] + bits[2]
    second = bits[0][:1] + bits[2] + bits[0][1:] + bits[1]
    return first, second


def to_stream(x, sizes):
    n = sizes[0] * sizes[1] * sizes[2]
    lead, total = x.shape[:-1], x.shape[-1]
    half = total // n // 2
    names = [(i, k) for i, m in enumerate(sizes) for k in reversed(range(m.bit_length() - 1))]
    y = x.reshape(lead + (2,) * len(names) + (2, half))
    parts = []
    for t, order in enumerate(stage_orders(sizes)):
        z = y[..., t, :]
        axes = (list(range(len(lead))) + [len(lead) + names.index(q) for q in order]
                + [z.ndim - 1])
        parts.append(jnp.transpose(z, axes).reshape(lead + (n * half,)))
    return jnp.concatenate(parts, axis=-1)


def short_kernel(sizes, basis_count, norm_atoms, norm_k,
                 table_ref, extra_ref, part_ref, kf_ref, nbr_ref, geo_ref, dy_ref, mix_ref,
                 gain_ref, shift_ref, dk_ref, dkt_ref,
                 home_ref, homex_ref, coefs_ref, fg_ref, weight_ref, radial_ref, own_ref,
                 halo, oh, near, filt, vals, ht, zg, acc, agg, gout, psum, rad,
                 grad, back, rb, sb, rf, sf, total, gbuf, wx, wy, wz, wout,
                 hs, hr, bs, br, rss, rsr, ags, agr, wss, wsr):
    n = sizes[0] * sizes[1] * sizes[2]
    ep = oh.shape[1]
    nbr, atoms = nbr_ref.shape
    channels = dy_ref.shape[0]
    orders = stage_orders(sizes)
    stages = len(orders[0])
    enter(n, sizes)
    mine = [lax.axis_index(a) for a in AXES]

    def slot_of(o):
        return 9 * (o[0] + 1) + 3 * (o[1] + 1) + o[2] + 1

    steps = [o for o in OFFSETS if o != (0, 0, 0)]
    halos = [remote(table_ref.at[tuple(own_span(d) for d in o)],
                    halo.at[tuple(span(d) for d in o)],
                    hs.at[slot_of(o)], hr.at[slot_of(o)], neighbour(o, sizes, -1))
             for o in steps]
    for copy in halos:
        copy.start()

    def bit_of(t, s):
        axis, k = orders[t][s]
        b = (mine[axis] // (2 ** k)) % 2
        to = tuple(m + (1 - 2 * b) * (2 ** k) if i == axis else m for i, m in enumerate(mine))
        return b, to

    lows = []
    for t in range(2):
        low = [0]
        for s in range(stages):
            low.append(low[-1] + bit_of(t, s)[0] * (n >> (s + 1)))
        lows.append(low)

    wide = [s for s in range(stages) if (n >> (s + 1)) <= 2]

    def place_of(s):
        if s in wide:
            return sum(n >> (q + 1) for q in wide if q < s)
        return sum(n >> (q + 1) for q in range(s))

    def scatter_copy(t, s):
        half = n >> (s + 1)
        b, to = bit_of(t, s)
        at = pl.ds(place_of(s), half)
        if s in wide:
            src, dst = sf.at[t, at], rf.at[t, at]
        else:
            src = part_ref.at[t, pl.ds((1 - b) * half, half)] if s == 0 else sb.at[t, at]
            dst = rb.at[t, at]
        return remote(src, dst, rss.at[t * stages + s], rsr.at[t * stages + s], to)

    def scatter_start(s):
        half = n >> (s + 1)
        for t in range(2):
            b, _ = bit_of(t, s)
            if s > 0:
                out = sf if s in wide else sb

                def fill(i, _, t=t, b=b, out=out):
                    out[t, place_of(s) + i] = total[t, (1 - b) * half + i].astype(out.dtype)
                    return 0

                lax.fori_loop(0, half, fill, 0)
            scatter_copy(t, s).start()

    def scatter_end(s):
        half = n >> (s + 1)
        for t in range(2):
            b, _ = bit_of(t, s)
            scatter_copy(t, s).wait()
            got = rf if s in wide else rb
            old = part_ref if s == 0 else total

            def fold(i, _, t=t, b=b, got=got, old=old):
                total[t, i] = (old[t, b * half + i].astype(f32)
                               + got[t, place_of(s) + i].astype(f32))
                return 0

            lax.fori_loop(0, half, fold, 0)

    def gather_copy(t, s):
        held = n >> (s + 1)
        _, to = bit_of(t, s)
        part = gbuf.at[t, pl.ds(lows[t][s + 1], held)]
        return remote(part, part, ags.at[t * stages + s], agr.at[t * stages + s], to)

    scatter_start(0)
    for copy in halos:
        copy.wait()
    halo[1:4, 1:4, 1:4] = table_ref[...]
    cells = 125 * 16
    extras = extra_ref.shape[0] * 16
    pad = ep - cells - extras
    table = jnp.concatenate(
        [halo[...].reshape(cells, LANES), extra_ref[...].reshape(extras, LANES),
         jnp.zeros((pad, LANES), bf16)], axis=0)
    tf = table.astype(f32)
    label = tf[:, LABEL:LABEL + 1]
    gtable = jnp.concatenate(
        [gain_ref[...], jnp.ones((gain_ref.shape[0], LANES - channels), f32)], axis=1)
    gains = jnp.zeros((ep, LANES), f32)
    for s in range(gain_ref.shape[0]):
        gains = jnp.where(label == float(s), gtable[s:s + 1, :], gains)
    zg[...] = gains
    mix = jnp.concatenate(
        [jnp.concatenate([mix_ref[...], jnp.zeros((channels, LANES - channels), bf16)], axis=1),
         jnp.zeros((LANES - channels, LANES), bf16)], axis=0)
    z = dot(table, mix) * gains
    lane = lax.broadcasted_iota(jnp.int32, (ep, LANES), 1)
    full = jnp.where(lane < channels, z, tf) + shift_ref[...]
    vals[...] = jnp.transpose(full).astype(bf16)
    ht[...] = jnp.transpose(tf).astype(bf16)
    spacing = reach_sq / (basis_count - 1)
    centre = lax.broadcasted_iota(jnp.int32, (basis_count, 1), 0).astype(f32) * spacing
    inv = 1.0 / (2.0 * spacing)
    own = geo_ref[0:8, :]
    agg[...] = jnp.zeros_like(agg)
    psum[...] = jnp.zeros_like(psum)
    acc[...] = jnp.zeros_like(acc)
    rad[...] = jnp.zeros_like(rad)
    one, nil = jnp.ones((), bf16), jnp.zeros((), bf16)
    dkt_hi, dkt_lo = split2(dkt_ref[...])
    dkt3 = jnp.concatenate([dkt_hi, dkt_lo, dkt_hi], axis=1)
    dk_hi, dk_lo = split2(dk_ref[...])
    dk3 = jnp.concatenate([dk_hi, dk_lo, dk_hi], axis=1)
    tile = 256

    def thirds(v):
        a = (v >= 9).astype(jnp.int32) + (v >= 18).astype(jnp.int32)
        r = v - 9 * a
        b = (r >= 3).astype(jnp.int32) + (r >= 6).astype(jnp.int32)
        return a, b, r - 3 * b

    def compact(e):
        slot = e // atoms
        atom = e - slot * atoms
        block = atom // 16
        o = thirds(slot)
        t = thirds(jnp.minimum(block, 26))
        x, y, w = [ti - 1 + 3 * (oi - 1) + 2 for ti, oi in zip(t, o)]
        cell = jnp.where(block < 27, 25 * x + 5 * y + w, 125 - 27 + block)
        return cell * 16 + (atom - block * 16)

    def geometry(j):
        at = near[j]
        place = at[POS_HI:POS_HI + 8] + at[POS_MID:POS_MID + 8] + at[POS_LO:POS_LO + 8]
        rel = (place + at[POS_OFF:POS_OFF + 8]) - own
        d2 = jnp.sum(rel * rel, axis=0, keepdims=True)
        arg = (d2 - centre) * inv
        return at, rel, arg, jnp.exp(-(arg * arg))

    def forward(j, _):
        cid = compact(nbr_ref[pl.ds(j, 1), :])
        high = cid // tile
        low = cid - high * tile
        for start in range(0, ep, tile):
            size = min(tile, ep - start)
            want = jnp.where(high == start // tile, low, -1).astype(f32).astype(bf16)
            rows = lax.broadcasted_iota(jnp.int32, (size, atoms), 0).astype(f32).astype(bf16)
            oh[j, start:start + size, :] = jnp.where(rows == want, one, nil)
        near[j] = dot(vals[0:GATHERED, :], oh[j])
        at, rel, arg, basis = geometry(j)
        b_hi, b_lo = split2(basis)
        f = dot(dkt3, jnp.concatenate([b_hi, b_hi, b_lo], axis=0))
        filt[j] = f
        agg[...] += f * at[0:channels]
        return 0

    cuts = [nbr * i // stages for i in range(stages + 1)]
    for s in range(stages):
        lax.fori_loop(cuts[s], cuts[s + 1], forward, 0)
        scatter_end(s)
        if s + 1 < stages:
            scatter_start(s + 1)
    ch = channels
    for t in range(2):
        rows = total[t, 0]
        hc = rows.shape[0]
        kf = kf_ref[t]
        cst = rows[:, 0:ch] * norm_atoms
        cbk = rows[:, ch:2 * ch] * norm_k
        sst = rows[:, 2 * ch:3 * ch] * norm_atoms
        sbk = rows[:, 3 * ch:4 * ch] * norm_k
        gbuf[t, lows[t][stages]] = jnp.concatenate(
            [norm_atoms * kf * cbk, norm_k * kf * cst, norm_atoms * kf * sbk,
             norm_k * kf * sst], axis=1).astype(bf16)
        fg_ref[t] = cst * cbk + sst * sbk
    for t in range(2):
        gather_copy(t, stages - 1).start()
    scale = nbr ** (-0.5)
    v = agg[...] * scale
    sg = 1.0 / (1.0 + jnp.exp(-v))
    gout[...] = dy_ref[...].astype(f32) * (sg * (1.0 + v * (1.0 - sg))) * scale

    def backward(j, _):
        g = gout[...]
        at, rel, arg, basis = geometry(j)
        dz = (filt[j] * g).astype(bf16)
        df_hi, df_lo = split2(at[0:channels] * g)
        db = dot(dk3, jnp.concatenate([df_hi, df_hi, df_lo], axis=0))
        dd2 = jnp.sum(db * basis * arg, axis=0, keepdims=True) * (-2.0 * inv)
        drel = 2.0 * rel * dd2
        psum[...] += drel
        d_hi = drel.astype(bf16).astype(f32)
        dvals = jnp.concatenate(
            [dz, jnp.concatenate([d_hi, drel - d_hi], axis=0).astype(bf16)], axis=0)
        acc[...] += dot_nt(oh[j], dvals)
        b_hi, b_lo = split2(basis)
        rad[...] += dot_nt(jnp.concatenate([b_hi, b_lo, b_hi], axis=1),
                           jnp.concatenate([df_hi, df_hi, df_lo], axis=1))
        return 0

    for i in range(stages):
        lax.fori_loop(cuts[i], cuts[i + 1], backward, 0)
        s = stages - 1 - i
        for t in range(2):
            gather_copy(t, s).wait()
            if s > 0:
                gather_copy(t, s - 1).start()
    g = acc[...]
    zgrad = g[:, 0:channels]
    pg = g[:, channels:channels + 8] + g[:, channels + 8:channels + 16]
    p_hi = pg.astype(bf16).astype(f32)
    rows = jnp.concatenate(
        [zgrad, p_hi, pg - p_hi, jnp.zeros((ep, LANES - channels - 16), f32)], axis=1)
    scaled = rows * zg[...]
    grad[...] = rows[0:cells].astype(bf16).reshape(grad.shape)
    returns = []
    for o in steps:
        loc = (slot_of(o),) + tuple(pl.ds(0, 3 if d == 0 else 1) for d in o)
        copy = remote(grad.at[tuple(span(d) for d in o)], back.at[loc],
                      bs.at[slot_of(o)], br.at[slot_of(o)], neighbour(o, sizes, 1))
        copy.start()
        returns.append(copy)
    homex_ref[...] = scaled[cells:cells + extras]
    own_ref[...] = psum[...]
    w = dot(ht[0:channels, :], scaled[:, 0:channels].astype(bf16))
    half = channels // 2
    r = rad[...]
    hb = basis_count // 2
    small = jnp.concatenate(
        [jnp.concatenate([w[:half], w[half:]], axis=1),
         jnp.concatenate([r[:hb], r[hb:]], axis=1)], axis=0)

    def small_start(axis, buf, value):
        count = sizes[axis]
        at = mine[axis]
        wout[axis] = value
        for i in range(1, count):
            to = tuple(lax.rem(m + i, count) if k == axis else m for k, m in enumerate(mine))
            remote(wout.at[axis], buf.at[at], wss.at[axis], wsr.at[axis], to).start()

    def small_end(axis, buf):
        count = sizes[axis]
        all_bytes(buf, count - 1, wss.at[axis]).wait()
        all_bytes(buf, count - 1, wsr.at[axis]).wait()
        buf[mine[axis]] = wout[axis]
        return jnp.sum(buf[...], axis=0)

    def land(group):
        for o, copy in group:
            copy.wait()
            at = tuple(slice(0, 3) if d == 0 else (slice(0, 1) if d > 0 else slice(2, 3))
                       for d in o)
            loc = (slot_of(o),) + tuple(slice(0, 3 if d == 0 else 1) for d in o)
            home_ref[at] += back[loc].astype(f32)

    pairs = sorted(zip(steps, returns), key=lambda p: sum(abs(d) for d in p[0]))
    small_start(0, wx, small)
    coefs_ref[...] = gbuf[...]
    home_ref[...] = rows[0:cells].reshape(grad.shape)[1:4, 1:4, 1:4]
    small = small_end(0, wx)
    small_start(1, wy, small)
    land(pairs[:6])
    small = small_end(1, wy)
    small_start(2, wz, small)
    land(pairs[6:])
    home_ref[...] *= zg[0:cells, :].reshape(5, 5, 5, 16, LANES)[1:4, 1:4, 1:4]
    small = small_end(2, wz)
    weight_ref[0:half] = small[0:half, 0:channels]
    weight_ref[half:channels] = small[0:half, channels:2 * channels]
    radial_ref[0:hb] = small[half:half + hb, 0:channels]
    radial_ref[hb:basis_count] = small[half:half + hb, channels:2 * channels]


def final_kernel(sizes, coef_ref, cos_ref, sin_ref, h_ref, dy_ref, milt_ref, home_ref,
                 extra_ref, own_ref, mix_ref, atom_ref, pos_ref, eh, ep_):
    rows = coef_ref.shape[0]
    channels, atoms = h_ref.shape
    step = 256
    stacked = jnp.concatenate([h_ref[...], dy_ref[...]], axis=0)
    eh[...] = jnp.zeros_like(eh)
    ep_[...] = jnp.zeros_like(ep_)

    def body(i, _):
        at = pl.ds(pl.multiple_of(i * step, step), step)
        piece = coef_ref[at, :]
        c, s = cos_ref[at, :], sin_ref[at, :]
        turned = jnp.transpose(piece.astype(f32)).astype(bf16)
        eh[...] += dot(turned[0:channels], c) + dot(turned[2 * channels:3 * channels], s)
        u = dot(piece[:, 0:2 * channels], stacked)
        v = dot(piece[:, 2 * channels:4 * channels], stacked)
        hi, lo = split2(v * c.astype(f32) - u * s.astype(f32))
        m = milt_ref[i]
        ep_[...] += dot(m, hi) + dot(m, lo)
        return 0

    lax.fori_loop(0, rows // step, body, 0)
    blocks = 27 * 16
    home = jnp.concatenate(
        [home_ref[...].reshape(blocks, LANES),
         extra_ref[...]], axis=0)
    g = jnp.transpose(home)
    zscaled = g[0:channels].astype(bf16)
    short = dot(mix_ref[...], zscaled)
    atom_ref[...] = (dy_ref[...].astype(f32) + eh[...] + short).astype(bf16)
    pos_short = g[channels:channels + 8] + g[channels + 8:channels + 16] - own_ref[...]
    pos_short = pos_short[0:3]
    for d in range(3):
        pos_ref[d:d + 1] = ep_[d:d + 1] * (2.0 * math.pi / sizes[d]) + pos_short[d:d + 1]


def vmem(count):
    return [pl.BlockSpec(memory_space=pltpu.VMEM)] * count


def params(**more):
    return pltpu.CompilerParams(vmem_limit_bytes=VMEM_LIMIT, **more)


def shards(sizes, atom_embedding, output_adjoint, fractional_coords, element_labels,
           adjacent_ghost_entries, miller_triples, reciprocal_kernel, channel_mixing_matrix,
           element_channel_factor, distance_kernel):
    n = sizes[0] * sizes[1] * sizes[2]
    shape = jax.ShapeDtypeStruct
    h = atom_embedding[0, 0, 0]
    dy = output_adjoint[0, 0, 0]
    pos = fractional_coords[0, 0, 0]
    channels, atoms = h.shape
    rows = miller_triples.shape[1]
    share = rows // n
    hs = share // 2
    basis_count = distance_kernel.shape[0]
    norm_atoms = (atoms * n) ** (-0.5)
    norm_k = rows ** (-0.5)
    counts = jnp.array(sizes, f32)
    anchor = jnp.stack([lax.axis_index(a) for a in AXES]).astype(f32)
    gap = jnp.zeros((5, atoms), f32)
    geo = jnp.concatenate(
        [pos, gap, (pos + anchor[:, None]) / counts[:, None], gap,
         element_labels[0, 0].astype(f32), jnp.zeros((7, atoms), f32)], axis=0)
    miller = to_stream(miller_triples.astype(f32), sizes)
    mil8 = jnp.pad(miller.T, ((0, 0), (0, 5)))
    extras = atoms // 16 - 27
    cos_all, sin_all, part, table, extra = pl.pallas_call(
        phase_kernel,
        out_shape=(shape((rows, atoms), bf16), shape((rows, atoms), bf16),
                   shape((rows, 4 * channels), bf16), shape((3, 3, 3, 16, LANES), bf16),
                   shape((extras, 16, LANES), bf16)),
        in_specs=vmem(4), out_specs=tuple(vmem(5)), compiler_params=params(), name="phases",
    )(h, dy, geo, mil8)

    me = lax.axis_index(AXES)
    kf = lax.dynamic_slice_in_dim(reciprocal_kernel, me * share, share, 0)
    dma = pltpu.SemaphoreType.DMA
    nbr = adjacent_ghost_entries.shape[3]
    ep = -(-((125 + extras) * 16) // LANES) * LANES
    shift = np.zeros((ep, LANES), np.float32)
    for i, cell in enumerate(itertools.product(range(5), repeat=3)):
        for d, q in enumerate(cell):
            shift[16 * i:16 * i + 16, POS_OFF + d] = -1.0 if q == 0 else (1.0 if q == 4 else 0.0)
    wr = channels // 2 + basis_count // 2
    stages = n.bit_length() - 1
    scratch = pltpu.VMEM
    home, homex, coefs, filter_share, weight_grad, radial_grad, own = pl.pallas_call(
        functools.partial(short_kernel, sizes, basis_count, norm_atoms, norm_k),
        out_shape=(shape((3, 3, 3, 16, LANES), f32), shape((extras * 16, LANES), f32),
                   shape((2, n, hs, 4 * channels), bf16), shape((2, hs, channels), f32),
                   shape((channels, channels), f32), shape((basis_count, channels), f32),
                   shape((8, atoms), f32)),
        in_specs=vmem(12), out_specs=tuple(vmem(7)),
        scratch_shapes=[scratch((5, 5, 5, 16, LANES), bf16),
                        scratch((nbr, ep, atoms), bf16),
                        scratch((nbr, GATHERED, atoms), f32),
                        scratch((nbr, channels, atoms), f32),
                        scratch((LANES, ep), bf16), scratch((LANES, ep), bf16),
                        scratch((ep, LANES), f32),
                        scratch((ep, channels + 16), f32),
                        scratch((channels, atoms), f32), scratch((channels, atoms), f32),
                        scratch((8, atoms), f32), scratch((basis_count, channels), f32),
                        scratch((5, 5, 5, 16, LANES), bf16),
                        scratch((27, 3, 3, 3, 16, LANES), bf16),
                        scratch((2, n, hs, 4 * channels), bf16),
                        scratch((2, n, hs, 4 * channels), bf16),
                        scratch((2, 4, hs, 4 * channels), f32),
                        scratch((2, 4, hs, 4 * channels), f32),
                        scratch((2, n // 2, hs, 4 * channels), f32),
                        scratch((2, n, hs, 4 * channels), bf16),
                        scratch((sizes[0], wr, LANES), f32),
                        scratch((sizes[1], wr, LANES), f32),
                        scratch((sizes[2], wr, LANES), f32),
                        scratch((3, wr, LANES), f32),
                        dma((27,)), dma((27,)), dma((27,)), dma((27,)),
                        dma((2 * stages,)), dma((2 * stages,)),
                        dma((2 * stages,)), dma((2 * stages,)), dma((3,)), dma((3,))],
        compiler_params=params(collective_id=0, has_side_effects=True), name="short",
    )(table, extra, part.reshape(2, n, hs, 4 * channels), kf.reshape(2, hs, channels),
      adjacent_ghost_entries[0, 0, 0], geo, dy, channel_mixing_matrix, element_channel_factor,
      jnp.asarray(shift), distance_kernel, distance_kernel.T)

    milt = jnp.pad(miller.astype(bf16), ((0, 13), (0, 0)))
    milt = jnp.transpose(milt.reshape(16, rows // 256, 256), (1, 0, 2))
    atom_grad, pos_grad = pl.pallas_call(
        functools.partial(final_kernel, sizes),
        out_shape=(shape((channels, atoms), bf16), shape((3, atoms), f32)),
        in_specs=vmem(10), out_specs=tuple(vmem(2)),
        scratch_shapes=[scratch((channels, atoms), f32), scratch((16, atoms), f32)],
        compiler_params=params(), name="final",
    )(coefs.reshape(rows, 4 * channels), cos_all, sin_all, h, dy, milt, home, homex, own,
      channel_mixing_matrix)
    return (atom_grad[None, None, None], pos_grad[None, None, None], weight_grad,
            radial_grad, filter_share.reshape(share, channels))


def solution(mesh):
    sizes = tuple(mesh.shape[a] for a in AXES)
    brick = P("gx", "gy", "gz", None, None)
    return jax.shard_map(
        functools.partial(shards, sizes),
        mesh=mesh,
        in_specs=(brick, brick, brick, P("gx", "gy", "gz", None), brick,
                  P(), P(), P(), P(), P()),
        out_specs=(brick, brick, P(), P(), P(("gx", "gy", "gz"), None)),
        check_vma=False,
    )
```
